256 devices in a mesh: owner: 8 (over x, core), rows: 32 (over z, y).
Axes of the slice: x: 4, y: 4, z: 8, core: 2. Of those that a mesh axis runs over, the one named last changes fastest.
Arguments:
- w_down: float32 [16, 6400, 4096], P('owner', None, 'rows'), may hold values from -0.15625 to 0.15625
- avg_down: bfloat16 [16, 6400, 4096], P('owner', None, 'rows'), may hold values from -0.0390625 to 0.0390625
- router_weight: float32 [4096, 16], P('rows', 'owner'), may hold values from -0.09375 to 0.09375
- router_gain: float32 [4096], P('rows'), may hold values from 0.25 to 1.75
Outputs:
- serve_down: bfloat16 [16, 6400, 4096], P('owner', 'rows')
- scale_down: float32 [16, 6400], P('owner', 'rows')
- serve_router: bfloat16 [4096, 16], replicated
The draws below stay inside these ranges and needn't reach their ends.
All inputs are finite; a program needn't handle non-finite values. Where the reference program divides by a largest or mean magnitude, that divisor is 1e-20 or more.
Results may differ from the reference program's by a relative error of at most 0.001.
Values may be sent and summed in bfloat16 or wider, within the bound.
No kernel may reach another device: no remote copies, remote signals or barrier semaphores. Data moves between devices by JAX's collectives and lax.ppermute only.
A program may use at most 64 MiB of HBM per device.

```python
import jax
import jax.numpy as jnp

EXPERTS = 16
D_MODEL = 4096
D_EXPERT = 6400


def strengthened(values, stream_key, source, target, parts, factor):
    def block_of(position):
        return (jnp.arange(values.shape[position]) // (values.shape[position] // parts)).reshape((-1,) + (1,) * (values.ndim - 1 - position))

    one_side = jax.random.permutation(stream_key, parts)[block_of(target)]
    second = (block_of(target) + parts // 2) % parts
    return jnp.where((block_of(source) == one_side) | (block_of(source) == second), factor * values, values)


def shard_levels(rng, dims, cuts, least, high):
    loudness = 1.0
    for dim, parts in cuts:
        draws = jax.random.uniform(jax.random.fold_in(jax.random.fold_in(rng, 6), dim), (parts,), jnp.float32, least / len(cuts), high / len(cuts))
        loudness = loudness * jnp.repeat(jnp.exp(draws), dims[dim] // parts).reshape((-1,) + (1,) * (len(dims) - 1 - dim))
    return loudness


def centred(key, extent, deviation, reach, shards=(), held_as=jnp.bfloat16):
    level = shard_levels(key, extent, shards, -0.22, 0.18) if shards else 1.0
    array = jax.random.normal(key, extent, jnp.float32) * deviation * level
    return jnp.minimum(jnp.maximum(array, -reach), reach).astype(held_as)


def bell_draw_with(stream_key, dims, width, limit, shards, heavy, dtype=jnp.bfloat16):
    result = width * jax.random.normal(stream_key, dims, jnp.float32)
    if shards:
        result = result * shard_levels(stream_key, dims, shards, -0.22, 0.18)
    return jnp.clip(strengthened(result, jax.random.fold_in(stream_key, 3), *heavy), -limit, limit).astype(dtype)


def setup_inputs(seed: int = 0) -> dict:
    seeds = jax.random.split(jax.random.key(seed), 5)
    w_down = bell_draw_with(seeds[0], (EXPERTS, D_EXPERT, D_MODEL), D_EXPERT ** -0.5, 0.15625, ((0, 8), (2, 32)), (2, 1, 32, 2.75), jnp.float32)
    avg_down = centred(seeds[1], (EXPERTS, D_EXPERT, D_MODEL), (D_EXPERT * 4) ** -0.5, 0.0390625, ((0, 8), (2, 32)))
    router_weight = centred(seeds[2], (D_MODEL, EXPERTS), D_MODEL ** -0.5, 0.09375, ((0, 32), (1, 8)), jnp.float32)
    router_gain = jnp.clip(1.0 + 0.15 * jax.random.normal(seeds[3], (D_MODEL,), jnp.float32), 0.25, 1.75)
    return dict(w_down=w_down, avg_down=avg_down, router_weight=router_weight, router_gain=router_gain)


def reference(w_down, avg_down, router_weight, router_gain):
    fresh_down = w_down + avg_down.astype(jnp.float32)
    scale_down = jnp.sum(jnp.abs(fresh_down), axis=2) / D_MODEL
    serve_down = (fresh_down / jnp.expand_dims(scale_down, 2)).astype(jnp.bfloat16)
    serve_router = (router_weight * router_gain[:, None]).astype(jnp.bfloat16)
    return serve_down, scale_down, serve_router
```

```python
import jax
import jax.numpy as jnp
from jax import lax
from jax.experimental import pallas as pl
from jax.experimental.pallas import tpu as pltpu
from jax.sharding import PartitionSpec as P

D_MODEL = 4096
LANES = 128
STEP = 40
BITS = 10
FINE = 8.0
SPAN = 239.0
MID = 120.0
ROOM = 24 * 2**20


def lane_of(shape):
    return lax.broadcasted_iota(jnp.int32, shape, len(shape) - 1)


def encode_kernel(w_ref, a_ref, o_ref):
    fresh = w_ref[...] + a_ref[...].astype(jnp.float32)
    size = jnp.abs(fresh)
    top = jnp.max(size, axis=-1, keepdims=True)
    level = jnp.clip(jnp.floor(FINE * (-2.0 - jnp.log2(top))), 0.0, 880.0)
    place = size * (jnp.exp2(2.0 + level * (1.0 / FINE)) * SPAN)
    lane = lane_of((1, 1, 1, LANES))
    digit = jnp.floor(level * jnp.exp2(-jnp.minimum(lane, BITS).astype(jnp.float32)))
    digit = digit - 2.0 * jnp.floor(digit * 0.5)
    marked = jnp.floor(place * 32.0 + 0.5) * (1.0 / 32.0) + digit * (1.0 / 64.0)
    place = jnp.where(lane < BITS, marked, place)
    code = jnp.exp2(place - MID)
    o_ref[...] = jnp.swapaxes(jnp.where(fresh < 0.0, -code, code).astype(jnp.bfloat16), 0, 1)


def encode(w, a):
    experts, count, rows, width = w.shape
    group = 2
    spec = pl.BlockSpec((experts, group, rows, width), lambda d: (0, d, 0, 0))
    return pl.pallas_call(
        encode_kernel,
        grid=(count // group,),
        in_specs=[spec, spec],
        out_specs=pl.BlockSpec((group, experts, rows, width), lambda d: (d, 0, 0, 0)),
        out_shape=jax.ShapeDtypeStruct((count, experts, rows, width), jnp.bfloat16),
        cost_estimate=pl.CostEstimate(flops=w.size * 30, transcendentals=0, bytes_accessed=w.size * 8),
        name="encode",
    )(w, a)


def decode_kernel(c_ref, d_ref, s_ref):
    count, _, rows, _ = c_ref.shape
    expert, step = pl.program_id(0), pl.program_id(1)
    lane = lane_of((1, 1, LANES))
    weight = jnp.where(lane < BITS, jnp.exp2(lane.astype(jnp.float32)), 0.0)
    wide = lax.broadcasted_iota(jnp.int32, (8, 256), 1)
    row = lax.broadcasted_iota(jnp.int32, (8, 256), 0)
    spread = jnp.zeros((8, 256), jnp.float32)
    for r in range(0, STEP, 8):
        start = pl.multiple_of(step * STEP + r, 8)
        code = c_ref[:, expert, pl.ds(start, 8), :].astype(jnp.float32)
        place = jnp.log2(jnp.abs(code)) + MID
        units = jnp.floor(place * 64.0 + 0.5)
        half = jnp.floor(units * 0.5)
        level = jnp.sum((units - 2.0 * half) * weight, axis=-1, keepdims=True)
        place = jnp.where(lane < BITS, half * (1.0 / 32.0), place)
        size = place * (jnp.exp2(-2.0 - level * (1.0 / FINE)) * (1.0 / SPAN))
        scale = jnp.sum(jnp.sum(size, axis=0), axis=-1, keepdims=True) * (1.0 / D_MODEL)
        value = jnp.where(code < 0.0, -size, size) / scale
        value = value.astype(jnp.bfloat16)
        for s in range(count):
            d_ref[0, r : r + 8, s * LANES : (s + 1) * LANES] = value[s]
        spread = jnp.where(wide == row + start, scale, spread)
    line = jnp.sum(spread, axis=0, keepdims=True)[:, :rows]
    here = lax.broadcasted_iota(jnp.int32, s_ref.shape, 1) - step * STEP
    mine = lax.broadcasted_iota(jnp.int32, s_ref.shape, 0) == expert
    s_ref[...] = jnp.where(mine & (here >= 0) & (here < STEP), line, s_ref[...])


def decode(code):
    count, experts, rows, width = code.shape
    return pl.pallas_call(
        decode_kernel,
        grid=(experts, rows // STEP),
        in_specs=[pl.BlockSpec(memory_space=pltpu.VMEM)],
        out_specs=[
            pl.BlockSpec((1, STEP, count * width), lambda e, r: (e, r, 0)),
            pl.BlockSpec((experts, rows), lambda e, r: (0, 0)),
        ],
        out_shape=[
            jax.ShapeDtypeStruct((experts, rows, count * width), jnp.bfloat16),
            jax.ShapeDtypeStruct((experts, rows), jnp.float32),
        ],
        cost_estimate=pl.CostEstimate(flops=code.size * 30, transcendentals=0, bytes_accessed=code.size * 4),
        compiler_params=pltpu.CompilerParams(vmem_limit_bytes=ROOM),
        name="decode",
    )(code)


def per_device(w_down, avg_down, router_weight, router_gain):
    experts, inner, width = w_down.shape
    count = lax.axis_size("rows")
    blocks = (experts, count, inner // count, width)
    code = lax.all_to_all(encode(w_down.reshape(blocks), avg_down.reshape(blocks)), "rows", 0, 0, tiled=True)
    serve, scale = decode(code)

    part = (router_weight * router_gain[:, None]).astype(jnp.bfloat16).T
    router = lax.all_gather(part, ("owner", "rows"), axis=0)
    router = router.reshape(-1, count, *part.shape).transpose(1, 3, 0, 2)
    return serve, scale, router.reshape(D_MODEL, -1)


def solution(mesh):
    return jax.shard_map(
        per_device,
        mesh=mesh,
        in_specs=(
            P("owner", None, "rows"),
            P("owner", None, "rows"),
            P("rows", "owner"),
            P("rows"),
        ),
        out_specs=(P("owner", "rows", None), P("owner", "rows"), P()),
        check_vma=False,
    )
```
